32 devices in a mesh: dp: 2 (over x), expert: 8 (over z, core), tensor: 2 (over y).
Axes of the slice: x: 2, y: 2, z: 4, core: 2. Of those that a mesh axis runs over, the one named last changes fastest.
Arguments:
- tokens: bfloat16 [192, 256, 1280], P(('dp', 'expert', 'tensor')), may hold values from -16 to 16
- cotangent: bfloat16 [192, 256, 1280], P(('dp', 'expert', 'tensor')), may hold values from -6 to 6
- norm_gain: float32 [1280], replicated, may hold values from 0.5 to 1.5
- slot_keys: bfloat16 [1280, 16], replicated, may hold values from -2 to 2
- w_in: bfloat16 [8, 1280, 2560], P('expert', None, 'tensor'), may hold values from -0.15625 to 0.15625
- w_out: bfloat16 [8, 2560, 1280], P('expert', 'tensor'), may hold values from -0.125 to 0.125
Outputs:
- grad_tokens: bfloat16 [192, 256, 1280], P(('dp', 'expert', 'tensor'))
- grad_gain: float32 [1280], replicated
- grad_keys: float32 [1280, 16], replicated
- grad_in: bfloat16 [8, 1280, 2560], P('expert', 'dp', 'tensor')
- grad_out: bfloat16 [8, 2560, 1280], P('expert', 'tensor', 'dp')
The draws below stay inside these ranges and needn't reach their ends.
All inputs are finite; a program needn't handle non-finite values.
Results may differ from the reference program's by a relative error of at most 0.014.
The reference program's roundings to bfloat16 on the way count: a program that leaves them out, or rounds other values in their place, can miss the bound.
Values may be sent and summed in bfloat16 or wider, within the bound.
A program may use at most 128 MiB of HBM per device.

```python
import math
import jax
import jax.numpy as jnp
from jax import lax

D = 1280
TOK_IMG = 256
SLOT_PER = 2
FF = 2560
IMG_DEV = 6
EXPERTS = 8
SLOTS = 16
IMAGES = 192


def draw_slot_keys(key, part):
    values = jax.random.normal(jax.random.fold_in(key, 11), (D, SLOTS), jnp.float32) * (1.0 / math.sqrt(D))
    limit = 1.0 + 2000 // D
    return jnp.clip(values, -limit, limit).astype(jnp.bfloat16)


def draw_tokens(key, part):
    values = jax.random.normal(jax.random.fold_in(key, 21), (IMAGES, TOK_IMG, D), jnp.float32)
    return jnp.clip(values, -16.0, 16.0).astype(jnp.bfloat16)


def level_of(rng, shape, split, smallest, largest):
    factor_of = 1.0
    for dim, blocks in split:
        draws = jax.random.uniform(jax.random.fold_in(jax.random.fold_in(rng, 6), dim), (blocks,), jnp.float32, smallest / len(split), largest / len(split))
        factor_of = factor_of * jnp.repeat(jnp.exp(draws), shape[dim] // blocks).reshape((-1,) + (1,) * (len(shape) - 1 - dim))
    return factor_of


def bell_draw(rng, extent, scale, most, split=(), dtype=jnp.bfloat16):
    values = scale * jax.random.normal(rng, extent, jnp.float32)
    if split:
        values = values * level_of(rng, extent, split, -0.22, 0.18)
    return jnp.clip(values, -most, most).astype(dtype)


def setup_inputs(seed: int = 0) -> dict:
    arg_keys = jax.random.split(jax.random.key(seed), 7)
    tokens = draw_tokens(jax.random.fold_in(arg_keys[6], 71), 0)
    cotangent = bell_draw(arg_keys[1], (IMAGES, TOK_IMG, D), 1.0, 6.0, ((0, 32),))
    norm_gain = jnp.clip(1.0 + 0.1 * jax.random.normal(arg_keys[2], (D,), jnp.float32), 0.5, 1.5)
    slot_keys = draw_slot_keys(jax.random.fold_in(arg_keys[6], 71), 0)
    w_in = bell_draw(arg_keys[4], (EXPERTS, D, FF), D ** -0.5, 0.15625, ((0, 8), (2, 2)))
    w_out = bell_draw(arg_keys[5], (EXPERTS, FF, D), FF ** -0.5, 0.125, ((0, 8), (1, 2)))
    return dict(tokens=tokens, cotangent=cotangent, norm_gain=norm_gain, slot_keys=slot_keys, w_in=w_in, w_out=w_out)


EPSILON = 1e-06

def rounded(values):
    lowered = lax.optimization_barrier(values.astype(jnp.bfloat16))
    return values + lax.stop_gradient(lowered.astype(jnp.float32) - values)

def mixing(tokens_wide, gain, keys_wide):
    average = lax.optimization_barrier(jnp.mean(tokens_wide, axis=-1, keepdims=True))
    centred = tokens_wide - average
    spread = lax.optimization_barrier(jnp.mean(centred * centred, axis=-1, keepdims=True))
    normed = rounded(centred * lax.rsqrt(spread + EPSILON) * gain)
    logits = jnp.einsum('bmd,dn->bmn', normed, keys_wide, precision=lax.Precision.HIGHEST)
    dispatch = rounded(jax.nn.softmax(logits, axis=1))
    combine = jax.nn.softmax(logits, axis=2)
    slot_values = jnp.einsum('bmn,bmd->bnd', dispatch, normed, precision=lax.Precision.HIGHEST)
    return (slot_values, combine)

def expert_forward(slot_rows, first_proj, second_proj):
    pre_act = jnp.dot(slot_rows.astype(jnp.float32), first_proj.astype(jnp.float32), preferred_element_type=jnp.float32)
    hidden = jax.nn.gelu(pre_act).astype(jnp.bfloat16)
    return jnp.dot(hidden.astype(jnp.float32), second_proj.astype(jnp.float32), preferred_element_type=jnp.float32).astype(jnp.bfloat16)

def expert_backward(slot_rows, row_grads, first_proj, second_proj):
    pre_act = jnp.dot(slot_rows.astype(jnp.float32), first_proj.astype(jnp.float32), preferred_element_type=jnp.float32)
    hidden = jax.nn.gelu(pre_act).astype(jnp.bfloat16)
    grad_hidden = lax.dot_general(row_grads.astype(jnp.float32), second_proj.astype(jnp.float32), (((1,), (1,)), ((), ())), preferred_element_type=jnp.float32)
    grad_pre = jax.vjp(jax.nn.gelu, pre_act)[1](grad_hidden)[0].astype(jnp.bfloat16)
    grad_rows = lax.dot_general(grad_pre.astype(jnp.float32), first_proj.astype(jnp.float32), (((1,), (1,)), ((), ())), preferred_element_type=jnp.float32)
    grad_first = lax.dot_general(slot_rows.astype(jnp.float32), grad_pre.astype(jnp.float32), (((0,), (0,)), ((), ())), preferred_element_type=jnp.float32)
    grad_second = lax.dot_general(hidden.astype(jnp.float32), row_grads.astype(jnp.float32), (((0,), (0,)), ((), ())), preferred_element_type=jnp.float32)
    return (grad_rows.astype(jnp.bfloat16), grad_first.astype(jnp.bfloat16), grad_second.astype(jnp.bfloat16))

def to_experts(per_image, images):
    experts = SLOTS // SLOT_PER
    shaped = per_image.reshape(images, experts, SLOT_PER, D)
    return jnp.transpose(shaped, (1, 0, 2, 3)).reshape(experts, images * SLOT_PER, D)

def from_experts(per_expert, images):
    experts = SLOTS // SLOT_PER
    shaped = per_expert.reshape(experts, images, SLOT_PER, D)
    return jnp.transpose(shaped, (1, 0, 2, 3)).reshape(images // IMG_DEV, IMG_DEV, SLOTS, D)

def reference(tokens, cotangent, norm_gain, slot_keys, w_in, w_out):
    images = tokens.shape[0]
    groups = images // IMG_DEV
    image_blocks = tokens.reshape(groups, IMG_DEV, TOK_IMG, D)
    grad_blocks = cotangent.reshape(groups, IMG_DEV, TOK_IMG, D)
    keys_wide = slot_keys.astype(jnp.float32)

    def forward_block(image_block):
        slot_values, combine = mixing(image_block.astype(jnp.float32), norm_gain, keys_wide)
        return (slot_values.astype(jnp.bfloat16), combine.astype(jnp.bfloat16))
    slot_inputs, combine_low = lax.map(forward_block, image_blocks)
    expert_rows = to_experts(slot_inputs, images)
    slot_outputs = lax.map(lambda inputs: expert_forward(inputs[0], inputs[1], inputs[2]), (expert_rows, w_in, w_out))
    slot_outputs = from_experts(slot_outputs, images)

    def combine_block(inputs):
        comb_block, grad_block, out_block = inputs
        grad_slots = jnp.einsum('bmn,bmd->bnd', comb_block.astype(jnp.float32), grad_block.astype(jnp.float32))
        grad_combine = jnp.einsum('bmd,bnd->bmn', grad_block.astype(jnp.float32), out_block.astype(jnp.float32))
        return (grad_slots.astype(jnp.bfloat16), grad_combine)
    grad_slots, grad_combine = lax.map(combine_block, (combine_low, grad_blocks, slot_outputs))
    grad_rows_in = to_experts(grad_slots, images)
    grad_rows, grad_first, grad_second = lax.map(lambda inputs: expert_backward(inputs[0], inputs[1], inputs[2], inputs[3]), (expert_rows, grad_rows_in, w_in, w_out))
    grad_slot_in = from_experts(grad_rows, images)

    def mixing_back(totals, inputs):
        image_block, grad_block, slot_grad, comb_grad = inputs
        unused, pullback = jax.vjp(mixing, image_block.astype(jnp.float32), norm_gain, keys_wide)
        grad_tok, grad_gain, grad_keys = pullback((slot_grad.astype(jnp.float32), comb_grad))
        result = (grad_block.astype(jnp.float32) + grad_tok).astype(jnp.bfloat16)
        return ((totals[0] + grad_gain, totals[1] + grad_keys), result)
    start_totals = (jnp.zeros((D,), jnp.float32), jnp.zeros((D, SLOTS), jnp.float32))
    totals, grad_tokens = lax.scan(mixing_back, start_totals, (image_blocks, grad_blocks, grad_slot_in, grad_combine))
    return (grad_tokens.reshape(images, TOK_IMG, D), totals[0], totals[1], grad_first, grad_second)
```

```python
import jax
import jax.numpy as jnp
from jax import lax
from jax.experimental import pallas as pl
from jax.experimental.pallas import tpu as pltpu
import functools
from jax.sharding import PartitionSpec as P

SLOT_PER = 2


EPSILON = 1e-06


def mixing_forward(tokens, gain, slot_keys):
    average = jnp.mean(tokens, axis=-1, keepdims=True, dtype=jnp.float32)
    centred = tokens.astype(jnp.float32) - average
    spread = jnp.mean(centred * centred, axis=-1, keepdims=True)
    inverse = lax.rsqrt(spread + EPSILON)
    scaled = centred * inverse
    normed = (scaled * gain).astype(jnp.bfloat16)
    logits = jnp.einsum("bmd,dn->bmn", normed, slot_keys, preferred_element_type=jnp.float32)
    dispatch = jax.nn.softmax(logits, axis=1)
    combine = jax.nn.softmax(logits, axis=2)
    dispatch_low = dispatch.astype(jnp.bfloat16)
    slot_values = jnp.einsum(
        "bmn,bmd->bnd", dispatch_low, normed, preferred_element_type=jnp.float32
    )
    return (slot_values, combine, (scaled, inverse, normed, dispatch, combine, dispatch_low))


def mixing_backward(saved, gain, slot_keys, slot_grad, combine_grad):
    scaled, inverse, normed, dispatch, combine, dispatch_low = saved
    grad_dispatch = jnp.einsum(
        "bnd,bmd->bmn", slot_grad, normed, preferred_element_type=jnp.float32
    )
    grad_normed = jnp.einsum(
        "bmn,bnd->bmd", dispatch_low, slot_grad, preferred_element_type=jnp.float32
    )
    grad_logits = dispatch * (
        grad_dispatch - jnp.sum(dispatch * grad_dispatch, axis=1, keepdims=True)
    )
    grad_logits = grad_logits + combine * (
        combine_grad - jnp.sum(combine * combine_grad, axis=2, keepdims=True)
    )
    keys_wide = slot_keys.astype(jnp.float32)
    grad_normed = grad_normed + jnp.einsum(
        "bmn,dn->bmd", grad_logits, keys_wide, precision=lax.Precision.HIGHEST
    )
    keys_term = jnp.einsum(
        "bmd,bmn->dn", normed.astype(jnp.float32), grad_logits, precision=lax.Precision.HIGHEST
    )
    gain_term = jnp.sum(grad_normed * scaled, axis=(0, 1))
    grad_scaled = grad_normed * gain
    first_mean = jnp.mean(grad_scaled, axis=-1, keepdims=True)
    second_mean = jnp.mean(grad_scaled * scaled, axis=-1, keepdims=True)
    grad_tok = inverse * (grad_scaled - first_mean - scaled * second_mean)
    return (grad_tok, gain_term, keys_term)


def contract_rows(left, right):
    return lax.dot_general(
        left, right, (((0,), (0,)), ((), ())), preferred_element_type=jnp.float32
    )


def contract_cols(left, right):
    return lax.dot_general(
        left, right, (((1,), (1,)), ((), ())), preferred_element_type=jnp.float32
    )


MESH = pl.DeviceIdType.MESH
AXES = ("dp", "expert", "tensor")
GELU_A = 0.7978845608028654
GELU_B = 0.044715
TILE = 256


def gelu_of(x):
    return 0.5 * x * (1.0 + jnp.tanh(GELU_A * (x + GELU_B * (x * x * x))))


def gelu_slope(x):
    square = x * x
    bend = jnp.tanh(GELU_A * (x + GELU_B * (square * x)))
    return 0.5 * (1.0 + bend) + 0.5 * x * (1.0 - bend * bend) * (
        GELU_A * (1.0 + 3.0 * GELU_B * square)
    )


def experts_kernel(dp, experts, tensor, spread, blk, w1, w2, back, s_all, g_all, h_all, p_all,
                   rows, s32, g32, pre, part, sent, got, pair, ret,
                   zs, zr, ys, yr, xs, xr, ps, pr, bs, br):
    d, e, t = (lax.axis_index(name) for name in AXES)
    height = blk.shape[1]
    half = height // 2
    own = experts * half
    group = tensor * own
    width = blk.shape[2]
    units = w1.shape[1]

    def around(position, step, size):
        return lax.rem(position + (step + size), size)

    def push(src, dst, send, recv, axis, where):
        target = {"dp": d, "expert": e, "tensor": t}
        target[axis] = where
        return pltpu.make_async_remote_copy(
            src_ref=src, dst_ref=dst, send_sem=send, recv_sem=recv,
            device_id=tuple(target[name] for name in AXES), device_id_type=MESH,
        )

    barrier = pltpu.get_barrier_semaphore()
    peers = [("expert", e, experts), ("tensor", t, tensor)] + ([("dp", d, dp)] if spread > 1 else [])
    count = 0
    for axis, place, size in peers:
        for k in range(1, size):
            target = {"dp": d, "expert": e, "tensor": t}
            target[axis] = around(place, k, size)
            pl.semaphore_signal(barrier, inc=1, device_id=tuple(target[n] for n in AXES), device_id_type=MESH)
            count += 1
    pl.semaphore_wait(barrier, count)

    mine = d if spread > 1 else 0
    started = []

    def launch(copy):
        copy.start()
        started.append(copy)

    arrive = [None] * experts
    for k in sorted(range(1, experts), key=lambda k: -min(k, experts - k)):
        to = around(e, k, experts)
        arrive[k] = push(blk.at[to], rows.at[mine, t, e], zs.at[k], zr.at[k], "expert", to)
        launch(arrive[k])

    def spread_y(src, k):
        slot = rows.at[mine, t, around(e, -k, experts)]
        for j in range(1, tensor):
            launch(push(src, slot, ys.at[j, k], yr.at[j, k], "tensor", around(t, j, tensor)))

    def spread_x(src, j, k):
        if spread > 1:
            slot = rows.at[mine, around(t, -j, tensor), around(e, -k, experts)]
            for i in range(1, dp):
                launch(push(src, slot, xs.at[j, i, k], xr.at[j, i, k], "dp", around(d, i, dp)))

    spread_y(blk.at[e], 0)
    spread_x(blk.at[e], 0, 0)
    rows[mine, t, e] = blk[e]
    near = sorted(range(1, experts), key=lambda k: -min(k, experts - k))
    for k in near:
        arrive[k].wait_recv()
        slot = rows.at[mine, t, around(e, -k, experts)]
        spread_y(slot, k)
        spread_x(slot, 0, k)
    for k in [0] + near:
        for j in range(1, tensor):
            slot = rows.at[mine, around(t, -j, tensor), around(e, -k, experts)]
            push(slot, slot, ys.at[j, k], yr.at[j, k], "tensor", around(t, j, tensor)).wait_recv()
            spread_x(slot, j, k)

    def unpack(where, base):
        count = tensor * experts
        for n in range(count):
            s32[pl.ds(half * n, height), :] = rows[where, n // experts, n % experts].astype(jnp.float32)
        lead = (-half) % 8
        for n in reversed(range(count)):
            g32[pl.ds(half * n + lead, height), :] = rows[where, n // experts, n % experts].astype(jnp.float32)
        s_all[pl.ds(base, group), :] = s32[0:group, :].astype(jnp.bfloat16)
        g_all[pl.ds(base, group), :] = g32[half + lead:half + lead + group, :].astype(jnp.bfloat16)

    def forward(base):
        @pl.loop(0, units // TILE)
        def _(n):
            cols = pl.ds(pl.multiple_of(n * TILE, TILE), TILE)
            x = jnp.dot(s_all[pl.ds(base, group), :], w1[:, cols], preferred_element_type=jnp.float32)
            pre[:, cols] = x
            h_all[pl.ds(base, group), cols] = gelu_of(x).astype(jnp.bfloat16)

    def backward(base):
        @pl.loop(0, units // TILE)
        def _(n):
            cols = pl.ds(pl.multiple_of(n * TILE, TILE), TILE)
            x = contract_cols(g_all[pl.ds(base, group), :], w2[cols, :])
            p_all[pl.ds(base, group), cols] = (x * gelu_slope(pre[:, cols])).astype(jnp.bfloat16)

    def share(which):
        for j in range(1, tensor):
            to = around(t, j, tensor)
            sent[which, j - 1] = part[which, pl.ds(pl.multiple_of(to * own, 8), own), :].astype(jnp.bfloat16)
            launch(push(sent.at[which, j - 1], got.at[which, j - 1], ps.at[which, j], pr.at[which, j], "tensor", to))

    base = 0
    unpack(mine, base)
    forward(base)

    @pl.loop(0, width // TILE)
    def _(n):
        cols = pl.ds(pl.multiple_of(n * TILE, TILE), TILE)
        part[0, :, cols] = jnp.dot(h_all[0:group, :], w2[:, cols], preferred_element_type=jnp.float32)

    share(0)
    backward(base)

    @pl.loop(0, width // TILE)
    def _(n):
        cols = pl.ds(pl.multiple_of(n * TILE, TILE), TILE)
        part[1, :, cols] = contract_cols(p_all[0:group, :], w1[cols, :])

    share(1)
    for which in range(2):
        total = part[which, pl.ds(pl.multiple_of(t * own, 8), own), :]
        for j in range(1, tensor):
            push(got.at[which, j - 1], got.at[which, j - 1], ps.at[which, j], pr.at[which, j],
                 "tensor", around(t, j, tensor)).wait_recv()
            total = total + got[which, j - 1].astype(jnp.float32)
        (s32 if which == 0 else g32)[0:own, :] = total
    for n in range(experts):
        pair[0:half, :] = s32[half * n:half * n + half, :]
        pair[half:height, :] = g32[half * n:half * n + half, :]
        ret[n] = pair[...].astype(jnp.bfloat16)
    backs = []
    for k in near:
        to = around(e, k, experts)
        backs.append(push(ret.at[to], back.at[e], bs.at[k], br.at[k], "expert", to))
        launch(backs[-1])
    back[e] = ret[e]
    if spread > 1:
        for i in range(1, dp):
            other = around(d, -i, dp)
            for j in range(tensor):
                for k in range(experts):
                    slot = rows.at[other, around(t, -j, tensor), around(e, -k, experts)]
                    push(slot, slot, xs.at[j, i, k], xr.at[j, i, k], "dp", around(d, i, dp)).wait_recv()
            unpack(other, i * group)
            forward(i * group)
            backward(i * group)
    for copy in backs:
        copy.wait_recv()
    for copy in started:
        copy.wait_send()


def run_experts(blk, w1, w2, dp, experts, tensor):
    height, width = blk.shape[1:]
    units = w1.shape[1]
    spread = dp if dp <= 2 else 1
    group = tensor * experts * (height // 2)
    own = experts * (height // 2)
    total = spread * group
    low, wide = jnp.bfloat16, jnp.float32
    dma = pltpu.SemaphoreType.DMA
    vm = pl.BlockSpec(memory_space=pltpu.VMEM)
    return pl.pallas_call(
        functools.partial(experts_kernel, dp, experts, tensor, spread),
        out_shape=(
            jax.ShapeDtypeStruct(blk.shape, low),
            jax.ShapeDtypeStruct((total, width), low),
            jax.ShapeDtypeStruct((total, width), low),
            jax.ShapeDtypeStruct((total, units), low),
            jax.ShapeDtypeStruct((total, units), low),
        ),
        in_specs=[vm] * 3,
        out_specs=[vm] * 5,
        scratch_shapes=[
            pltpu.VMEM((spread, tensor, experts, height, width), low),
            pltpu.VMEM((group + 2 * height, width), wide),
            pltpu.VMEM((group + 2 * height, width), wide),
            pltpu.VMEM((group, units), wide),
            pltpu.VMEM((2, group, width), wide),
            pltpu.VMEM((2, max(tensor - 1, 1), own, width), low),
            pltpu.VMEM((2, max(tensor - 1, 1), own, width), low),
            pltpu.VMEM((height, width), wide),
            pltpu.VMEM((experts, height, width), low),
            dma((experts,)), dma((experts,)),
            dma((tensor, experts)), dma((tensor, experts)),
            dma((tensor, dp, experts)), dma((tensor, dp, experts)),
            dma((2, tensor)), dma((2, tensor)),
            dma((experts,)), dma((experts,)),
        ],
        compiler_params=pltpu.CompilerParams(
            collective_id=0, has_side_effects=True, vmem_limit_bytes=60 * 1024 * 1024
        ),
        name="experts",
    )(blk, w1, w2)


def reduce_kernel(sizes, x, out, got, total, ss, sr, gs, gr):
    where = [lax.axis_index(name) for name in AXES]
    count = sizes[0] * sizes[1] * sizes[2]
    me = (where[0] * sizes[1] + where[1]) * sizes[2] + where[2]

    def device(index):
        return (index // (sizes[1] * sizes[2]), (index // sizes[2]) % sizes[1], index % sizes[2])

    def later(k):
        return lax.rem(me + k, count)

    def scatter(k):
        to = later(k)
        return pltpu.make_async_remote_copy(
            src_ref=x.at[to], dst_ref=got.at[k], send_sem=ss.at[k], recv_sem=sr.at[k],
            device_id=device(to), device_id_type=MESH)

    def gather(k):
        to = later(k)
        return pltpu.make_async_remote_copy(
            src_ref=total, dst_ref=out.at[me], send_sem=gs.at[k], recv_sem=gr.at[k],
            device_id=device(to), device_id_type=MESH)

    def each(body):
        def step(k, carry):
            body(k)
            return carry
        lax.fori_loop(1, count, step, 0)

    barrier = pltpu.get_barrier_semaphore()
    each(lambda k: pl.semaphore_signal(barrier, inc=1, device_id=device(later(k)), device_id_type=MESH))
    pl.semaphore_wait(barrier, count - 1)
    each(lambda k: scatter(k).start())
    got[0] = x[me]
    each(lambda k: scatter(k).wait_recv())
    total[...] = jnp.sum(got[...], axis=0)
    each(lambda k: gather(k).start())
    out[me] = total[...]
    each(lambda k: gather(k).wait_recv())
    each(lambda k: scatter(k).wait_send())
    each(lambda k: gather(k).wait_send())


def reduce_all(values, sizes):
    count = sizes[0] * sizes[1] * sizes[2]
    flat = jnp.concatenate([v.reshape(-1) for v in values])
    chunk = -(-flat.shape[0] // (count * 1024)) * 1024
    packed = jnp.pad(flat, (0, count * chunk - flat.shape[0])).reshape(count, chunk // 128, 128)
    vm = pl.BlockSpec(memory_space=pltpu.VMEM)
    dma = pltpu.SemaphoreType.DMA
    summed = pl.pallas_call(
        functools.partial(reduce_kernel, sizes),
        out_shape=jax.ShapeDtypeStruct(packed.shape, jnp.float32),
        in_specs=[vm],
        out_specs=vm,
        scratch_shapes=[
            pltpu.VMEM(packed.shape, jnp.float32),
            pltpu.VMEM(packed.shape[1:], jnp.float32),
            dma((count,)), dma((count,)), dma((count,)), dma((count,)),
        ],
        compiler_params=pltpu.CompilerParams(collective_id=1, has_side_effects=True),
        name="reduce",
    )(packed).reshape(-1)
    results, start = [], 0
    for v in values:
        results.append(summed[start:start + v.size].reshape(v.shape))
        start += v.size
    return results


def local(sizes, tokens, cotangent, norm_gain, slot_keys, w_in, w_out):
    dp, experts, tensor = sizes
    local_imgs, token_count, features = tokens.shape
    slot_count = slot_keys.shape[1]
    slot_values, combine, saved = mixing_forward(tokens, norm_gain, slot_keys)
    combine_low = combine.astype(jnp.bfloat16)
    grad_slots = jnp.einsum(
        "bmn,bmd->bnd", combine_low, cotangent, preferred_element_type=jnp.float32
    )
    both = jnp.stack([slot_values.astype(jnp.bfloat16), grad_slots.astype(jnp.bfloat16)])
    both = both.reshape(2, local_imgs, experts, SLOT_PER, features)
    blk = both.transpose(2, 0, 1, 3, 4).reshape(experts, 2 * local_imgs * SLOT_PER, features)
    back, slot_rows, grad_rows, hidden, grad_pre = run_experts(
        blk, w_in[0], w_out[0], dp, experts, tensor
    )
    back = back.reshape(experts, 2, local_imgs, SLOT_PER, features).transpose(1, 2, 0, 3, 4)
    back = back.reshape(2, local_imgs, slot_count, features)
    returned, grad_back = back[0], back[1]
    if dp > 2:
        slot_rows = lax.all_to_all(slot_rows, "dp", split_axis=1, concat_axis=0, tiled=True)
        grad_rows = lax.all_to_all(grad_rows, "dp", split_axis=1, concat_axis=0, tiled=True)
        hidden = lax.all_gather(hidden, "dp", axis=0, tiled=True)
        grad_pre = lax.all_gather(grad_pre, "dp", axis=0, tiled=True)
    else:
        width = features // dp
        start = lax.axis_index("dp") * width
        slot_rows = lax.dynamic_slice_in_dim(slot_rows, start, width, axis=1)
        grad_rows = lax.dynamic_slice_in_dim(grad_rows, start, width, axis=1)
    first_total = contract_rows(slot_rows, grad_pre)
    second_total = contract_rows(hidden, grad_rows)
    grad_combine = jnp.einsum(
        "bmd,bnd->bmn", cotangent, returned, preferred_element_type=jnp.float32
    )
    grad_tok, gain_term, keys_term = mixing_backward(
        saved, norm_gain, slot_keys, grad_back, grad_combine
    )
    grad_tokens = (cotangent.astype(jnp.float32) + grad_tok).astype(jnp.bfloat16)
    grad_gain, grad_keys = reduce_all((gain_term, keys_term), sizes)
    return (
        grad_tokens,
        grad_gain,
        grad_keys,
        first_total.astype(jnp.bfloat16)[None],
        second_total.astype(jnp.bfloat16)[None],
    )


def solution(mesh):
    placed = (
        P(("dp", "expert", "tensor"), None, None),
        P(("dp", "expert", "tensor"), None, None),
        P(),
        P(),
        P("expert", None, "tensor"),
        P("expert", "tensor", None),
    )
    return jax.shard_map(
        functools.partial(local, tuple(mesh.shape[name] for name in AXES)),
        mesh=mesh,
        in_specs=placed,
        out_specs=(
            P(("dp", "expert", "tensor"), None, None),
            P(),
            P(),
            P("expert", "dp", "tensor"),
            P("expert", "tensor", "dp"),
        ),
        check_vma=False,
    )
```

```python
import jax
import jax.numpy as jnp
from jax import lax
from jax.experimental import pallas as pl
from jax.experimental.pallas import tpu as pltpu
import functools
import numpy as np
from jax.sharding import PartitionSpec as P

SLOT_PER = 2


EPSILON = 1e-06


CHUNK = 64


def mix_kernel(x, c, gain, keys, perm, normed, disp, comb, stat, blk, stack):
    b = pl.program_id(0)
    slots = keys.shape[0]
    images = pl.num_programs(0)
    gains = gain[...]

    def rows_of(n, carry):
        rows = pl.ds(pl.multiple_of(n * CHUNK, CHUNK), CHUNK)
        values = x[0, rows, :].astype(jnp.float32)
        average = jnp.mean(values, axis=-1, keepdims=True)
        centred = values - average
        inverse = lax.rsqrt(jnp.mean(centred * centred, axis=-1, keepdims=True) + EPSILON)
        normed[0, rows, :] = (centred * inverse * gains).astype(jnp.bfloat16)
        lane = lax.broadcasted_iota(jnp.int32, (CHUNK, stat.shape[2]), 1)
        stat[0, rows, :] = jnp.where(lane == 0, average, inverse)
        return carry

    lax.fori_loop(0, x.shape[1] // CHUNK, rows_of, 0)
    logits = contract_cols(keys[...], normed[0])
    over_tokens = jnp.exp(logits - jnp.max(logits, axis=1, keepdims=True))
    over_tokens = over_tokens / jnp.sum(over_tokens, axis=1, keepdims=True)
    over_slots = jnp.exp(logits - jnp.max(logits, axis=0, keepdims=True))
    over_slots = over_slots / jnp.sum(over_slots, axis=0, keepdims=True)
    disp[0] = over_tokens
    comb[0] = over_slots
    start = pl.multiple_of(b * slots, slots)
    stack[0, pl.ds(start, slots), :] = jnp.dot(
        over_tokens.astype(jnp.bfloat16), normed[0], preferred_element_type=jnp.float32
    ).astype(jnp.bfloat16)
    stack[1, pl.ds(start, slots), :] = jnp.dot(
        over_slots.astype(jnp.bfloat16), c[0], preferred_element_type=jnp.float32
    ).astype(jnp.bfloat16)

    @pl.when(b == images - 1)
    def _():
        height = blk.shape[1]
        count = stack.shape[1]
        moved = jnp.dot(perm[:, 0:count], stack[0], preferred_element_type=jnp.float32)
        moved = moved + jnp.dot(perm[:, count:2 * count], stack[1], preferred_element_type=jnp.float32)
        for n in range(blk.shape[0]):
            blk[n] = moved[n * height:(n + 1) * height].astype(jnp.bfloat16)


def placement(images, experts):
    slots = experts * SLOT_PER
    height = 2 * images * SLOT_PER
    r = np.arange(experts * height)
    e, q = r // height, r % height
    stream, u = q // (images * SLOT_PER), q % (images * SLOT_PER)
    return stream, u // SLOT_PER, e * SLOT_PER + u % SLOT_PER, slots


def mix(tokens, cotangent, gain, keys, experts):
    images, count, features = tokens.shape
    stream, image, slot, slots = placement(images, experts)
    perm = np.zeros((stream.size, stream.size), np.float32)
    perm[np.arange(stream.size), stream * images * slots + image * slots + slot] = 1.0
    height = 2 * images * SLOT_PER
    per_image = lambda *tail: pl.BlockSpec((1,) + tail, lambda b: (b, 0, 0))
    whole = lambda *shape: pl.BlockSpec(shape, lambda b: (0,) * len(shape))
    low, wide = jnp.bfloat16, jnp.float32
    return pl.pallas_call(
        mix_kernel,
        grid=(images,),
        out_shape=(
            jax.ShapeDtypeStruct(tokens.shape, low),
            jax.ShapeDtypeStruct((images, slots, count), wide),
            jax.ShapeDtypeStruct((images, slots, count), wide),
            jax.ShapeDtypeStruct((images, count, 128), wide),
            jax.ShapeDtypeStruct((experts, height, features), low),
        ),
        in_specs=[
            per_image(count, features), per_image(count, features), whole(1, features),
            whole(slots, features), whole(*perm.shape),
        ],
        out_specs=(
            per_image(count, features), per_image(slots, count), per_image(slots, count),
            per_image(count, 128), whole(experts, height, features),
        ),
        scratch_shapes=[pltpu.VMEM((2, images * slots, features), low)],
        compiler_params=pltpu.CompilerParams(vmem_limit_bytes=32 * 1024 * 1024),
        name="mix",
    )(tokens, cotangent, gain, keys, jnp.asarray(perm, low))


def unmix_kernel(x, c, normed, disp, comb, stat, gain, keys, sel, back, out, gain_out, keys_out,
                 grad, gain_sum):
    b = pl.program_id(0)
    slots = keys.shape[0]
    low = jnp.bfloat16
    got = jnp.dot(sel[0], back[...], preferred_element_type=jnp.float32).astype(low)
    returned, slot_grad = got[0:slots], got[slots:2 * slots]
    grad_dispatch = contract_cols(slot_grad, normed[0])
    grad_combine = contract_cols(returned, c[0])
    dispatch, combine = disp[0], comb[0]
    logit = dispatch * (
        grad_dispatch - jnp.sum(dispatch * grad_dispatch, axis=1, keepdims=True)
    ) + combine * (grad_combine - jnp.sum(combine * grad_combine, axis=0, keepdims=True))
    first = logit.astype(low)
    rest = logit - first.astype(jnp.float32)
    second = rest.astype(low)
    third = (rest - second.astype(jnp.float32)).astype(low)
    key = keys[...]
    left = jnp.concatenate([dispatch.astype(low), first, second, third], axis=0)
    right = jnp.concatenate([slot_grad, key, key, key], axis=0)
    grad[...] = contract_rows(left, right)
    parts = jnp.dot(left[slots:], normed[0], preferred_element_type=jnp.float32)
    keys_here = parts[0:slots] + parts[slots:2 * slots] + parts[2 * slots:3 * slots]

    @pl.when(b == 0)
    def _():
        keys_out[...] = jnp.zeros_like(keys_out)
        gain_sum[...] = jnp.zeros_like(gain_sum)

    keys_out[...] += keys_here
    gains = gain[...]

    def rows_of(n, total):
        rows = pl.ds(pl.multiple_of(n * CHUNK, CHUNK), CHUNK)
        average, inverse = stat[0, rows, 0:1], stat[0, rows, 1:2]
        scaled = (x[0, rows, :].astype(jnp.float32) - average) * inverse
        grads = grad[rows, :]
        product = grads * scaled
        total = total + sum(product[k:k + 8] for k in range(0, CHUNK, 8))
        grads = grads * gains
        first_mean = jnp.mean(grads, axis=-1, keepdims=True)
        second_mean = jnp.mean(product * gains, axis=-1, keepdims=True)
        change = inverse * (grads - first_mean - scaled * second_mean)
        out[0, rows, :] = (c[0, rows, :].astype(jnp.float32) + change).astype(low)
        return total

    gain_sum[...] = lax.fori_loop(0, x.shape[1] // CHUNK, rows_of, gain_sum[...])

    @pl.when(b == pl.num_programs(0) - 1)
    def _():
        gain_out[...] = jnp.sum(gain_sum[...], axis=0, keepdims=True)


def unmix(tokens, cotangent, saved, gain, keys, back, experts):
    images, count, features = tokens.shape
    stream, image, slot, slots = placement(images, experts)
    sel = np.zeros((images, 2 * slots, stream.size), np.float32)
    sel[image, stream * slots + slot, np.arange(stream.size)] = 1.0
    normed, disp, comb, stat = saved
    per_image = lambda *tail: pl.BlockSpec((1,) + tail, lambda b: (b, 0, 0))
    whole = lambda *shape: pl.BlockSpec(shape, lambda b: (0,) * len(shape))
    return pl.pallas_call(
        unmix_kernel,
        grid=(images,),
        out_shape=(
            jax.ShapeDtypeStruct(tokens.shape, jnp.bfloat16),
            jax.ShapeDtypeStruct((1, features), jnp.float32),
            jax.ShapeDtypeStruct((slots, features), jnp.float32),
        ),
        in_specs=[
            per_image(count, features), per_image(count, features), per_image(count, features),
            per_image(slots, count), per_image(slots, count), per_image(count, 128),
            whole(1, features), whole(slots, features),
            per_image(2 * slots, stream.size), whole(stream.size, features),
        ],
        out_specs=(per_image(count, features), whole(1, features), whole(slots, features)),
        scratch_shapes=[
            pltpu.VMEM((count, features), jnp.float32), pltpu.VMEM((8, features), jnp.float32),
        ],
        compiler_params=pltpu.CompilerParams(vmem_limit_bytes=32 * 1024 * 1024),
        name="unmix",
    )(tokens, cotangent, normed, disp, comb, stat, gain, keys, jnp.asarray(sel, jnp.bfloat16), back)


def contract_rows(left, right):
    return lax.dot_general(
        left, right, (((0,), (0,)), ((), ())), preferred_element_type=jnp.float32
    )


def contract_cols(left, right):
    return lax.dot_general(
        left, right, (((1,), (1,)), ((), ())), preferred_element_type=jnp.float32
    )


MESH = pl.DeviceIdType.MESH
AXES = ("dp", "expert", "tensor")
GELU_A = 0.7978845608028654
GELU_B = 0.044715
TILE = 256


def gelu_of(x):
    return 0.5 * x * (1.0 + jnp.tanh(GELU_A * (x + GELU_B * (x * x * x))))


def gelu_slope(x):
    square = x * x
    bend = jnp.tanh(GELU_A * (x + GELU_B * (square * x)))
    return 0.5 * (1.0 + bend) + 0.5 * x * (1.0 - bend * bend) * (
        GELU_A * (1.0 + 3.0 * GELU_B * square)
    )


def experts_kernel(dp, experts, tensor, spread, finish, blk, w1, w2, back, *refs):
    if finish:
        grad_in, grad_out, turned, *refs = refs
    (s_all, g_all, h_all, p_all, rows, s32, g32, pre, part, sent, got, pair, ret,
     zs, zr, ys, yr, xs, xr, ps, pr, bs, br) = refs
    d, e, t = (lax.axis_index(name) for name in AXES)
    height = blk.shape[1]
    half = height // 2
    own = experts * half
    group = tensor * own
    width = blk.shape[2]
    units = w1.shape[1]

    def around(position, step, size):
        return lax.rem(position + (step + size), size)

    def push(src, dst, send, recv, axis, where):
        target = {"dp": d, "expert": e, "tensor": t}
        target[axis] = where
        return pltpu.make_async_remote_copy(
            src_ref=src, dst_ref=dst, send_sem=send, recv_sem=recv,
            device_id=tuple(target[name] for name in AXES), device_id_type=MESH,
        )

    barrier = pltpu.get_barrier_semaphore()
    peers = [("expert", e, experts), ("tensor", t, tensor)] + ([("dp", d, dp)] if spread > 1 else [])
    count = 0
    for axis, place, size in peers:
        for k in range(1, size):
            target = {"dp": d, "expert": e, "tensor": t}
            target[axis] = around(place, k, size)
            pl.semaphore_signal(barrier, inc=1, device_id=tuple(target[n] for n in AXES), device_id_type=MESH)
            count += 1
    pl.semaphore_wait(barrier, count)

    mine = d if spread > 1 else 0
    started = []

    def launch(copy):
        copy.start()
        started.append(copy)

    arrive = [None] * experts
    for k in sorted(range(1, experts), key=lambda k: -min(k, experts - k)):
        to = around(e, k, experts)
        arrive[k] = push(blk.at[to], rows.at[mine, t, e], zs.at[k], zr.at[k], "expert", to)
        launch(arrive[k])

    def spread_y(src, k):
        slot = rows.at[mine, t, around(e, -k, experts)]
        for j in range(1, tensor):
            launch(push(src, slot, ys.at[j, k], yr.at[j, k], "tensor", around(t, j, tensor)))

    def spread_x(src, j, k):
        if spread > 1:
            slot = rows.at[mine, around(t, -j, tensor), around(e, -k, experts)]
            for i in range(1, dp):
                launch(push(src, slot, xs.at[j, i, k], xr.at[j, i, k], "dp", around(d, i, dp)))

    spread_y(blk.at[e], 0)
    spread_x(blk.at[e], 0, 0)
    rows[mine, t, e] = blk[e]
    near = sorted(range(1, experts), key=lambda k: -min(k, experts - k))
    for k in near:
        arrive[k].wait_recv()
        slot = rows.at[mine, t, around(e, -k, experts)]
        spread_y(slot, k)
        spread_x(slot, 0, k)
    for k in [0] + near:
        for j in range(1, tensor):
            slot = rows.at[mine, around(t, -j, tensor), around(e, -k, experts)]
            push(slot, slot, ys.at[j, k], yr.at[j, k], "tensor", around(t, j, tensor)).wait_recv()
            spread_x(slot, j, k)

    def unpack(where, base):
        count = tensor * experts
        for n in range(count):
            s32[pl.ds(half * n, height), :] = rows[where, n // experts, n % experts].astype(jnp.float32)
        lead = (-half) % 8
        for n in reversed(range(count)):
            g32[pl.ds(half * n + lead, height), :] = rows[where, n // experts, n % experts].astype(jnp.float32)
        s_all[pl.ds(base, group), :] = s32[0:group, :].astype(jnp.bfloat16)
        g_all[pl.ds(base, group), :] = g32[half + lead:half + lead + group, :].astype(jnp.bfloat16)

    def forward(base):
        @pl.loop(0, units // TILE)
        def _(n):
            cols = pl.ds(pl.multiple_of(n * TILE, TILE), TILE)
            x = jnp.dot(s_all[pl.ds(base, group), :], w1[:, cols], preferred_element_type=jnp.float32)
            pre[:, cols] = x
            h_all[pl.ds(base, group), cols] = gelu_of(x).astype(jnp.bfloat16)

    def backward(base):
        @pl.loop(0, units // TILE)
        def _(n):
            cols = pl.ds(pl.multiple_of(n * TILE, TILE), TILE)
            x = contract_cols(g_all[pl.ds(base, group), :], w2[cols, :])
            p_all[pl.ds(base, group), cols] = (x * gelu_slope(pre[:, cols])).astype(jnp.bfloat16)

    def share(which):
        for j in range(1, tensor):
            to = around(t, j, tensor)
            sent[which, j - 1] = part[which, pl.ds(pl.multiple_of(to * own, 8), own), :].astype(jnp.bfloat16)
            launch(push(sent.at[which, j - 1], got.at[which, j - 1], ps.at[which, j], pr.at[which, j], "tensor", to))

    base = 0
    unpack(mine, base)
    forward(base)

    @pl.loop(0, width // TILE)
    def _(n):
        cols = pl.ds(pl.multiple_of(n * TILE, TILE), TILE)
        part[0, :, cols] = jnp.dot(h_all[0:group, :], w2[:, cols], preferred_element_type=jnp.float32)

    share(0)
    backward(base)

    @pl.loop(0, width // TILE)
    def _(n):
        cols = pl.ds(pl.multiple_of(n * TILE, TILE), TILE)
        part[1, :, cols] = contract_cols(p_all[0:group, :], w1[cols, :])

    share(1)
    for which in range(2):
        total = part[which, pl.ds(pl.multiple_of(t * own, 8), own), :]
        for j in range(1, tensor):
            push(got.at[which, j - 1], got.at[which, j - 1], ps.at[which, j], pr.at[which, j],
                 "tensor", around(t, j, tensor)).wait_recv()
            total = total + got[which, j - 1].astype(jnp.float32)
        (s32 if which == 0 else g32)[0:own, :] = total
    for n in range(experts):
        pair[0:half, :] = s32[half * n:half * n + half, :]
        pair[half:height, :] = g32[half * n:half * n + half, :]
        ret[n] = pair[...].astype(jnp.bfloat16)
    backs = []
    for k in near:
        to = around(e, k, experts)
        backs.append(push(ret.at[to], back.at[e], bs.at[k], br.at[k], "expert", to))
        launch(backs[-1])
    back[e] = ret[e]
    if spread > 1:
        for i in range(1, dp):
            other = around(d, -i, dp)
            for j in range(tensor):
                for k in range(experts):
                    slot = rows.at[other, around(t, -j, tensor), around(e, -k, experts)]
                    push(slot, slot, xs.at[j, i, k], xr.at[j, i, k], "dp", around(d, i, dp)).wait_recv()
            unpack(other, i * group)
            forward(i * group)
            backward(i * group)
    if finish:
        share_width = width // dp
        mine_cols = pl.ds(pl.multiple_of(d * share_width, 128), share_width)
        turned[...] = s_all[:, mine_cols].T

        @pl.loop(0, units // TILE)
        def _(n):
            cols = pl.ds(pl.multiple_of(n * TILE, TILE), TILE)
            grad_in[:, cols] = jnp.dot(
                turned[...], p_all[:, cols], preferred_element_type=jnp.float32
            ).astype(jnp.bfloat16)
            grad_out[cols, :] = contract_rows(h_all[:, cols], g_all[:, mine_cols]).astype(jnp.bfloat16)

    for copy in backs:
        copy.wait_recv()
    for copy in started:
        copy.wait_send()


def run_experts(blk, w1, w2, dp, experts, tensor):
    height, width = blk.shape[1:]
    units = w1.shape[1]
    spread = dp if dp <= 2 else 1
    group = tensor * experts * (height // 2)
    own = experts * (height // 2)
    total = spread * group
    low, wide = jnp.bfloat16, jnp.float32
    dma = pltpu.SemaphoreType.DMA
    vm = pl.BlockSpec(memory_space=pltpu.VMEM)
    shapes = [(total, width), (total, width), (total, units), (total, units)]
    finish = spread == dp and width % (128 * dp) == 0
    kept = [pltpu.VMEM(shape, low) for shape in shapes]
    if finish:
        shapes = [(width // dp, units), (units, width // dp)]
        kept = [pltpu.VMEM((width // dp, total), low)] + kept
    else:
        kept = []
    return pl.pallas_call(
        functools.partial(experts_kernel, dp, experts, tensor, spread, finish),
        out_shape=[jax.ShapeDtypeStruct(shape, low) for shape in [blk.shape] + shapes],
        in_specs=[vm] * 3,
        out_specs=[vm] * (1 + len(shapes)),
        scratch_shapes=kept + [
            pltpu.VMEM((spread, tensor, experts, height, width), low),
            pltpu.VMEM((group + 2 * height, width), wide),
            pltpu.VMEM((group + 2 * height, width), wide),
            pltpu.VMEM((group, units), wide),
            pltpu.VMEM((2, group, width), wide),
            pltpu.VMEM((2, max(tensor - 1, 1), own, width), low),
            pltpu.VMEM((2, max(tensor - 1, 1), own, width), low),
            pltpu.VMEM((height, width), wide),
            pltpu.VMEM((experts, height, width), low),
            dma((experts,)), dma((experts,)),
            dma((tensor, experts)), dma((tensor, experts)),
            dma((tensor, dp, experts)), dma((tensor, dp, experts)),
            dma((2, tensor)), dma((2, tensor)),
            dma((experts,)), dma((experts,)),
        ],
        compiler_params=pltpu.CompilerParams(
            collective_id=0, has_side_effects=True, vmem_limit_bytes=60 * 1024 * 1024
        ),
        name="experts",
    )(blk, w1, w2)


def reduce_kernel(sizes, x, out, got, total, ss, sr, gs, gr):
    where = [lax.axis_index(name) for name in AXES]
    table = [
        [place] + [lax.rem(place + k, size) for k in range(1, size)]
        for place, size in zip(where, sizes)
    ]
    targets = [(a, b, c) for a in table[0] for b in table[1] for c in table[2]]
    rank = lambda p: (p[0] * sizes[1] + p[1]) * sizes[2] + p[2]
    me = rank(where)
    others = range(1, len(targets))

    def scatter(k):
        return pltpu.make_async_remote_copy(
            src_ref=x.at[rank(targets[k])], dst_ref=got.at[k], send_sem=ss.at[k], recv_sem=sr.at[k],
            device_id=targets[k], device_id_type=MESH)

    def gather(k):
        return pltpu.make_async_remote_copy(
            src_ref=total, dst_ref=out.at[me], send_sem=gs.at[k], recv_sem=gr.at[k],
            device_id=targets[k], device_id_type=MESH)

    barrier = pltpu.get_barrier_semaphore()
    for k in others:
        pl.semaphore_signal(barrier, inc=1, device_id=targets[k], device_id_type=MESH)
    pl.semaphore_wait(barrier, len(others))
    first = [scatter(k) for k in others]
    for copy in first:
        copy.start()
    got[0] = x[me]
    for copy in first:
        copy.wait_recv()
    total[...] = jnp.sum(got[...], axis=0)
    second = [gather(k) for k in others]
    for copy in second:
        copy.start()
    out[me] = total[...]
    for copy in second:
        copy.wait_recv()
    for copy in first + second:
        copy.wait_send()


def reduce_all(values, sizes):
    count = sizes[0] * sizes[1] * sizes[2]
    flat = jnp.concatenate([v.reshape(-1) for v in values])
    chunk = -(-flat.shape[0] // (count * 1024)) * 1024
    packed = jnp.pad(flat, (0, count * chunk - flat.shape[0])).reshape(count, chunk // 128, 128)
    vm = pl.BlockSpec(memory_space=pltpu.VMEM)
    dma = pltpu.SemaphoreType.DMA
    summed = pl.pallas_call(
        functools.partial(reduce_kernel, sizes),
        out_shape=jax.ShapeDtypeStruct(packed.shape, jnp.float32),
        in_specs=[vm],
        out_specs=vm,
        scratch_shapes=[
            pltpu.VMEM(packed.shape, jnp.float32),
            pltpu.VMEM(packed.shape[1:], jnp.float32),
            dma((count,)), dma((count,)), dma((count,)), dma((count,)),
        ],
        compiler_params=pltpu.CompilerParams(collective_id=1, has_side_effects=True),
        name="reduce",
    )(packed).reshape(-1)
    results, start = [], 0
    for v in values:
        results.append(summed[start:start + v.size].reshape(v.shape))
        start += v.size
    return results


def local(sizes, tokens, cotangent, norm_gain, slot_keys, w_in, w_out):
    dp, experts, tensor = sizes
    features = tokens.shape[2]
    gain, keys = norm_gain.reshape(1, features), slot_keys.T
    *saved, blk = mix(tokens, cotangent, gain, keys, experts)
    back, *rest = run_experts(blk, w_in[0], w_out[0], dp, experts, tensor)
    if len(rest) == 2:
        first_total, second_total = rest
    else:
        slot_rows, grad_rows, hidden, grad_pre = rest
        if dp > 2:
            slot_rows = lax.all_to_all(slot_rows, "dp", split_axis=1, concat_axis=0, tiled=True)
            grad_rows = lax.all_to_all(grad_rows, "dp", split_axis=1, concat_axis=0, tiled=True)
            hidden = lax.all_gather(hidden, "dp", axis=0, tiled=True)
            grad_pre = lax.all_gather(grad_pre, "dp", axis=0, tiled=True)
        else:
            width = features // dp
            start = lax.axis_index("dp") * width
            slot_rows = lax.dynamic_slice_in_dim(slot_rows, start, width, axis=1)
            grad_rows = lax.dynamic_slice_in_dim(grad_rows, start, width, axis=1)
        first_total = contract_rows(slot_rows, grad_pre)
        second_total = contract_rows(hidden, grad_rows)
    grad_tokens, gain_term, keys_term = unmix(
        tokens, cotangent, saved, gain, keys, back.reshape(-1, features), experts
    )
    grad_gain, grad_keys = reduce_all((gain_term, keys_term), sizes)
    grad_gain, grad_keys = grad_gain.reshape(features), grad_keys.T
    return (
        grad_tokens,
        grad_gain,
        grad_keys,
        first_total.astype(jnp.bfloat16)[None],
        second_total.astype(jnp.bfloat16)[None],
    )


def solution(mesh):
    placed = (
        P(("dp", "expert", "tensor"), None, None),
        P(("dp", "expert", "tensor"), None, None),
        P(),
        P(),
        P("expert", None, "tensor"),
        P("expert", "tensor", None),
    )
    return jax.shard_map(
        functools.partial(local, tuple(mesh.shape[name] for name in AXES)),
        mesh=mesh,
        in_specs=placed,
        out_specs=(
            P(("dp", "expert", "tensor"), None, None),
            P(),
            P(),
            P("expert", "dp", "tensor"),
            P("expert", "tensor", "dp"),
        ),
        check_vma=False,
    )
```
